256 devices in a mesh: panel: 32 (over y, x, core), samp: 8 (over z).
Axes of the slice: x: 4, y: 4, z: 8, core: 2. Of those that a mesh axis runs over, the one named last changes fastest.
Arguments:
- called_allele_tallies: int32 [4096, 1024], P('samp'), may hold values from 0 to 2
- presence_flags: int32 [4096, 1024], P('samp'), may hold values 0 or 1
- reference_panel_strands: int32 [65536, 1024], P('panel'), may hold values from 0 to 1
- softmax_sharpness: float32 [4096], P('samp'), may hold values from 0.02 to 4
- trait_measurements: float32 [4096], P('samp'), may hold values from -8 to 8
- cohort_membership: int32 [4096], P('samp'), may hold values from 0 to 7, as said below
Outputs:
- dosage_out: bfloat16 [4096, 1024], P('samp', 'panel')
- zscore: float32 [1024], P('panel')
The draws below stay inside these ranges and needn't reach their ends.
Inputs may be any that keep to these rules, and one draw needn't show every extreme that they name: `cohort_membership`: every group id from 0 to 7 occurs.
All inputs are finite; a program needn't handle non-finite values. No bound on the sum of `presence_flags` on one device may be relied on, other than what follows from the above.
Results may differ from the reference program's by a relative error of at most 0.0055.
Values sent between devices are 32-bit elements; how exact they have to be, the bound alone decides.
No kernel may reach another device: no remote copies, remote signals or barrier semaphores. Data moves between devices by JAX's collectives and lax.ppermute only.
A program may use at most 64 MiB of HBM per device.

```python
import jax
import jax.numpy as jnp
from jax import lax

SPAN_MARKERS = 1024
GROUPS = 8
HAPLOTYPES = 65536
SAMPLES = 4096


def draw_reference_panel_strands(key, part):
    key_base = jax.random.fold_in(key, 11)
    key_noise = jax.random.fold_in(key, 12)
    base_level = jax.random.randint(key_base, (SPAN_MARKERS,), 100, 700)
    noise = jax.random.randint(key_noise, (HAPLOTYPES, SPAN_MARKERS), 0, 1000)
    rows = jnp.arange(HAPLOTYPES, dtype=jnp.int32)[:, None]
    bound = base_level[None, :] * (HAPLOTYPES + 2 * rows) // (3 * HAPLOTYPES)
    return (noise < bound).astype(jnp.int32)


def draw_softmax_sharpness(key, part):
    uniform_draw = jax.random.uniform(jax.random.fold_in(key, 21), (SAMPLES,), jnp.float32)
    values = jnp.exp(jnp.log(0.02) + uniform_draw * jnp.log(15.0))
    return values.astype(jnp.float32)


def draw_trait_measurements(key, part):
    rows = jnp.arange(SAMPLES, dtype=jnp.float32)
    ramp = 0.5 + 1.5 * rows / SAMPLES
    noise = jax.random.normal(jax.random.fold_in(key, 32), (SAMPLES,), jnp.float32)
    values = ramp * noise
    return jnp.clip(values, -8.0, 8.0).astype(jnp.float32)


def draw_cohort_membership(key, part):
    drawn = jax.random.randint(jax.random.fold_in(key, 41), (SAMPLES,), 0, GROUPS)
    rows = jnp.arange(SAMPLES, dtype=jnp.int32)
    return jnp.where(rows < GROUPS, rows, drawn).astype(jnp.int32)


def set_ends(values, stream_key, smallest, high):
    extent = values.shape
    index_at = [jax.random.randint(jax.random.fold_in(stream_key, axis), (), 0, extent[axis]) for axis in range(len(extent))]
    values = values.at[tuple(index_at)].set(smallest)
    longest = extent.index(max(extent))
    index_at[longest] = (index_at[longest] + 1) % extent[longest]
    return values.at[tuple(index_at)].set(high)


def setup_inputs(seed: int = 0) -> dict:
    splits = jax.random.split(jax.random.key(seed), 7)
    return {
        "called_allele_tallies": set_ends(jax.random.randint(splits[0], (SAMPLES, SPAN_MARKERS), 0, 3), jax.random.fold_in(splits[0], 1), 0, 2).astype(jnp.int32),
        "presence_flags": set_ends((jax.random.randint(splits[1], (SAMPLES, SPAN_MARKERS), 0, 4) < 3).astype(jnp.int32), jax.random.fold_in(splits[1], 1), 0, 1),
        "reference_panel_strands": draw_reference_panel_strands(jax.random.fold_in(splits[6], 71), 0),
        "softmax_sharpness": draw_softmax_sharpness(jax.random.fold_in(splits[6], 71), 0),
        "trait_measurements": draw_trait_measurements(jax.random.fold_in(splits[6], 71), 0),
        "cohort_membership": draw_cohort_membership(jax.random.fold_in(splits[6], 71), 0),
    }


log_two = 0.6931471805599453

def reference(called_allele_tallies, presence_flags, reference_panel_strands, softmax_sharpness, trait_measurements, cohort_membership):
    hap_float = reference_panel_strands.astype(jnp.float32)
    allele_freq = lax.optimization_barrier(jnp.sum(hap_float, axis=0)) / HAPLOTYPES
    geno_float = called_allele_tallies.astype(jnp.float32)
    observed_f = presence_flags.astype(jnp.float32)
    demeaned_expected_count = (observed_f * (geno_float - 2.0 * allele_freq[None, :])).astype(jnp.bfloat16)
    tile_first_entry = lax.optimization_barrier(jnp.sum(demeaned_expected_count.astype(jnp.float32) * allele_freq[None, :], axis=1))
    hap_bf = reference_panel_strands.astype(jnp.bfloat16)
    entries_in_tile = min(SAMPLES, 512)
    tile_ordinal = SAMPLES // entries_in_tile

    def whole_matrix_tile(pieces):
        cen, offset, heat = pieces
        raw_efficient_statistic = lax.dot_general(cen, hap_bf, (((1,), (1,)), ((), ())), preferred_element_type=jnp.float32)
        panel_match_energies = heat[:, None] * (raw_efficient_statistic - offset[:, None])
        peak_steps = jnp.ceil(lax.optimization_barrier(jnp.max(panel_match_energies, axis=1)) / log_two)
        weights = jnp.exp(panel_match_energies - log_two * peak_steps[:, None])
        weight_total = lax.optimization_barrier(jnp.sum(weights, axis=1))
        summed = jnp.dot(weights.astype(jnp.bfloat16), hap_bf, preferred_element_type=jnp.float32)
        return 2.0 * summed / weight_total[:, None]
    expected_allele_count = lax.map(whole_matrix_tile, (demeaned_expected_count.reshape(tile_ordinal, entries_in_tile, SPAN_MARKERS), tile_first_entry.reshape(tile_ordinal, entries_in_tile), softmax_sharpness.reshape(tile_ordinal, entries_in_tile)))
    expected_allele_count = expected_allele_count.reshape(SAMPLES, SPAN_MARKERS)
    dosage = jnp.where(presence_flags == 1, geno_float, expected_allele_count)
    dosage_out = dosage.astype(jnp.bfloat16)
    member = (cohort_membership[:, None] == jnp.arange(GROUPS, dtype=jnp.int32)[None, :]).astype(jnp.float32)
    group_sum = jnp.dot(trait_measurements, member, precision=lax.Precision.HIGHEST)
    group_count = lax.optimization_barrier(jnp.sum(member, axis=0))
    group_mean = group_sum / group_count
    resid = trait_measurements - jnp.dot(member, group_mean, precision=lax.Precision.HIGHEST)
    sigma = jnp.sum(resid * resid) / (SAMPLES - GROUPS)
    score_u = jnp.dot(resid, dosage, precision=lax.Precision.HIGHEST)
    dose_mean = lax.optimization_barrier(jnp.sum(dosage, axis=0)) / SAMPLES
    spread = lax.optimization_barrier(jnp.sum(dosage * dosage, axis=0)) / SAMPLES - dose_mean * dose_mean
    zscore = score_u / jnp.sqrt(sigma * SAMPLES * (spread + 1e-05))
    return (dosage_out, zscore)
```

```python
import functools

import jax
import jax.numpy as jnp
from jax import lax
from jax.experimental import pallas as pl
from jax.experimental.pallas import tpu as pltpu
from jax.sharding import Mesh
from jax.sharding import PartitionSpec as P

GROUPS = 8
CHIP_AXES = ("panel_0", "panel_1")
PANEL = ("panel_0", "panel_1", "panel_2")
LOG_TWO = 0.6931471805599453
LOG2_E = 1.4426950408889634
LANES = 128
STATS = 16
MIB = 1 << 20

VMEM = pltpu.VMEM


def in_vmem(x):
    return pltpu.with_memory_space_constraint(x, VMEM)


def whole():
    return pl.BlockSpec(memory_space=VMEM)


def count_kernel(panel, as_bf16, counts, landed, tile, sems):
    rows, variants = panel.shape
    pieces = sems.shape[0]
    step = rows // pieces

    def copy(i):
        span = pl.ds(i * step, step)
        return pltpu.make_async_copy(panel.at[span], landed.at[span], sems.at[i])

    for i in range(pieces):
        copy(i).start()

    total = jnp.zeros((8, variants), jnp.int32)
    for i in range(pieces):
        copy(i).wait()

        def body(r, acc):
            span = pl.ds(pl.multiple_of(i * step + r * 32, 32), 32)
            x = landed[span, :]
            as_bf16[span, :] = x.astype(jnp.float32).astype(jnp.bfloat16)
            return acc + jnp.sum(x.reshape(4, 8, variants), axis=0)

        total = lax.fori_loop(0, step // 32, body, total)
    row = jnp.sum(total.astype(jnp.float32), axis=0, keepdims=True)
    for r in range(variants // LANES):
        tile[r : r + 1, :] = row[:, r * LANES : (r + 1) * LANES]
    one = tile[...]
    for j in range(counts.shape[0]):
        counts[j] = one


def turn_kernel(as_bf16, called, present, turned, own, called_part, present_part, flipped, sems):
    haps, variants = as_bf16.shape
    core = lax.axis_index("panel_2")
    here = (lax.axis_index("panel_0") * lax.axis_size("panel_1") + lax.axis_index("panel_1")) * 2
    here = here + core
    share = own.shape[0]
    per_tile = LANES // share
    lanes = pl.ds(pl.multiple_of((here // per_tile) * LANES, LANES), LANES)
    first = pltpu.make_async_copy(called.at[:, lanes], called_part, sems.at[0])
    second = pltpu.make_async_copy(present.at[:, lanes], present_part, sems.at[1])
    first.start()
    second.start()
    half = variants // 2
    block = 256

    def body(h, carry):
        at = pl.ds(pl.multiple_of(h * block, block), block)
        for t in range(variants // LANES):
            x = as_bf16[at, t * LANES : (t + 1) * LANES].T
            for q in range(per_tile):
                chip = t * (per_tile // 2) + q // 2
                slot = jnp.bitwise_xor(core, q % 2)
                to = pl.ds(pl.multiple_of(slot * half + chip * share, share), share)
                turned[to, at] = x[q * share : (q + 1) * share, :]
        return carry

    lax.fori_loop(0, haps // block, body, 0)
    first.wait()
    second.wait()
    code = jnp.where(present_part[...] == 1, called_part[...].astype(jnp.float32), -1.0)
    flipped[...] = code.T
    own[...] = flipped[pl.ds(pl.multiple_of((here % per_tile) * share, share), share), :]


def impute_kernel(
    haplotypes,
    as_bf16,
    turned,
    counts,
    called,
    present,
    sharpness,
    mine,
    other,
    centred,
    offsets,
    raw,
    weights,
):
    samples, variants = called.shape
    haps = as_bf16.shape[0]
    tiles = samples // LANES
    total = jnp.sum(counts[...], axis=0)
    freq = jnp.concatenate([total[r : r + 1, :] for r in range(variants // LANES)], axis=1)
    freq = freq / haplotypes
    twice = 2.0 * freq

    step = 32

    def centre(r, carry):
        span = pl.ds(pl.multiple_of(r * step, step), step)
        c = present[span, :].astype(jnp.float32) * (called[span, :].astype(jnp.float32) - twice)
        c = c.astype(jnp.bfloat16)
        centred[span, :] = c
        off = jnp.sum(c.astype(jnp.float32) * freq, axis=1, keepdims=True)
        offsets[span, :] = jnp.broadcast_to(off, (step, LANES))
        return carry

    lax.fori_loop(0, samples // step, centre, 0)
    offset = jnp.concatenate(
        [offsets[t * LANES : (t + 1) * LANES, :].T[0:1, :] for t in range(tiles)], axis=1
    )

    raw[...] = lax.dot_general(
        as_bf16[...], centred[...], (((1,), (1,)), ((), ())), preferred_element_type=jnp.float32
    )

    chunk = 64

    def highest(r, best):
        x = raw[pl.ds(pl.multiple_of(r * chunk, chunk), chunk), :]
        return jnp.maximum(best, jnp.max(x.reshape(chunk // 8, 8, samples), axis=0))

    best = lax.fori_loop(
        0, haps // chunk, highest, jnp.full((8, samples), -jnp.inf, jnp.float32)
    )
    best = jnp.max(best, axis=0, keepdims=True)
    heat = sharpness[...]
    peak = heat * (best - offset)
    steps = jnp.ceil(peak / LOG_TWO)
    slope = heat * LOG2_E
    shift = peak * LOG2_E - steps

    def weigh(r, acc):
        span = pl.ds(pl.multiple_of(r * chunk, chunk), chunk)
        w = jnp.exp2(slope * (raw[span, :] - best) + shift)
        weights[span, :] = w.astype(jnp.bfloat16)
        return acc + jnp.sum(w.reshape(chunk // 8, 8, samples), axis=0)

    acc = lax.fori_loop(0, haps // chunk, weigh, jnp.zeros((8, samples), jnp.float32))
    weight_total = jnp.sum(acc, axis=0, keepdims=True)

    blocks = mine.shape[0]
    share = (mine.shape[1] - 2 * tiles) // tiles
    for out, start in ((mine, 0), (other, variants // 2)):
        dose = jnp.dot(
            turned[start : start + variants // 2, :],
            weights[...],
            preferred_element_type=jnp.float32,
        )
        for t in range(tiles):
            lanes = slice(t * LANES, (t + 1) * LANES)
            for k in range(blocks):
                out[k, t * share : (t + 1) * share, :] = dose[k * share : (k + 1) * share, lanes]
        for t in range(tiles):
            lanes = slice(t * LANES, (t + 1) * LANES)
            out[0, tiles * share + t : tiles * share + t + 1, :] = steps[:, lanes]
            out[0, tiles * (share + 1) + t : tiles * (share + 1) + t + 1, :] = weight_total[:, lanes]


def pair_kernel(mine, theirs, both):
    blocks, height, _ = mine.shape
    tiles = 4
    share = height // tiles - 2
    top = tiles * share
    a, b = mine[0, top : top + tiles, :], theirs[0, top : top + tiles, :]
    steps = jnp.maximum(a, b)
    up, down = jnp.exp2(a - steps), jnp.exp2(b - steps)
    total = up * mine[0, top + tiles :, :] + down * theirs[0, top + tiles :, :]
    tail = jnp.concatenate([steps, total], axis=0)
    for k in range(blocks):
        for t in range(tiles):
            span = slice(t * share, (t + 1) * share)
            both[k, span, :] = (
                mine[k, span, :] * up[t : t + 1, :] + theirs[k, span, :] * down[t : t + 1, :]
            )
        both[k, top:, :] = tail


def dose_kernel(parts, own, trait, cohort, dose_out, stats, square):
    blocks, height, _ = parts.shape
    tiles = 4
    share = height // tiles - 2
    top = tiles * share
    sums = [jnp.zeros((share, LANES), jnp.float32) for _ in range(3 + GROUPS)]
    tail = [jnp.zeros((GROUPS, LANES), jnp.float32) for _ in range(3)]
    row = lax.broadcasted_iota(jnp.int32, (GROUPS, LANES), 0)
    steps = jnp.max(parts[:, top : top + tiles, :], axis=0)
    for t in range(tiles):
        lanes = slice(t * LANES, (t + 1) * LANES)
        peak = steps[t : t + 1, :]
        total = jnp.zeros((1, LANES), jnp.float32)
        dose = jnp.zeros((share, LANES), jnp.float32)
        for k in range(blocks):
            scale = jnp.exp2(parts[k, top + t : top + t + 1, :] - peak)
            total += scale * parts[k, top + tiles + t : top + tiles + t + 1, :]
            dose += scale * parts[k, t * share : (t + 1) * share, :]
        called = own[:, lanes]
        dose = jnp.where(called >= 0.0, called, 2.0 * dose / total)
        dose_out[:, lanes] = dose.astype(jnp.bfloat16)
        y, group = trait[:, lanes], cohort[:, lanes]
        sums[0] += y * dose
        sums[1] += dose
        sums[2] += dose * dose
        for g in range(GROUPS):
            sums[3 + g] += jnp.where(group == g, dose, 0.0)
        member = jnp.where(group == row, 1.0, 0.0)
        tail[0] += member * y
        tail[1] += member
        tail[2] += jnp.where(row == 0, y * y, 0.0)
    square[...] = jnp.zeros_like(square)
    lane = lax.broadcasted_iota(jnp.int32, (share, LANES), 1)
    packed = jnp.zeros((share, LANES), jnp.float32)
    for i, s in enumerate(sums):
        packed = jnp.where(lane == i, jnp.sum(s, axis=1, keepdims=True), packed)
    square[0:share, :] = packed
    lane = lax.broadcasted_iota(jnp.int32, (GROUPS, LANES), 1)
    packed = square[0:GROUPS, :]
    for i, s in enumerate(tail):
        packed = jnp.where(lane == 3 + GROUPS + i, jnp.sum(s, axis=1, keepdims=True), packed)
    square[0:GROUPS, :] = packed
    flat = square[...].T[0:STATS, :]
    for j in range(stats.shape[0]):
        stats[j] = flat


def score_kernel(all_samples, stats, zscore):
    s = jnp.sum(stats[...], axis=0)
    cross, dose_sum, dose_square = s[0:1, :], s[1:2, :], s[2:3, :]
    group_dose = s[3 : 3 + GROUPS, :]
    group_sum, group_count = s[3 + GROUPS : 4 + GROUPS, :], s[4 + GROUPS : 5 + GROUPS, :]
    lane = lax.broadcasted_iota(jnp.int32, (1, LANES), 1)
    group_mean = jnp.where(
        lane < GROUPS, group_sum / jnp.where(lane < GROUPS, group_count, 1.0), 0.0
    )
    row = lax.broadcasted_iota(jnp.int32, (GROUPS, LANES), 0)
    col = lax.broadcasted_iota(jnp.int32, (GROUPS, LANES), 1)
    means = jnp.sum(jnp.where(row == col, group_mean, 0.0), axis=1, keepdims=True)
    score_u = cross - jnp.sum(means * group_dose, axis=0, keepdims=True)
    explained = jnp.sum(
        jnp.where(lane < GROUPS, group_sum * group_mean, 0.0), axis=1, keepdims=True
    )
    square = s[5 + GROUPS : 6 + GROUPS, 0:1]
    sigma = (square - explained) / (all_samples - GROUPS)
    mean = dose_sum / all_samples
    spread = dose_square / all_samples - mean * mean
    z = score_u / jnp.sqrt(sigma * all_samples * (spread + 1e-05))
    zscore[...] = z[:, : zscore.shape[1]]


def on_device(called, present, panel, sharpness, trait, cohort):
    f32, bf16 = jnp.float32, jnp.bfloat16
    samples, variants = called.shape
    haps = panel.shape[0]
    devices = lax.axis_size(PANEL)
    chips = lax.axis_size(CHIP_AXES)
    strata = lax.axis_size("samp")
    tiles = samples // LANES
    share = variants // devices
    height = tiles * (share + 2)
    pieces = 16

    as_bf16, counts = pl.pallas_call(
        count_kernel,
        out_shape=(VMEM((haps, variants), bf16), VMEM((devices, 8, LANES), f32)),
        in_specs=[pl.BlockSpec(memory_space=pl.ANY)],
        out_specs=(whole(), whole()),
        scratch_shapes=[
            VMEM((haps, variants), jnp.int32),
            VMEM((8, LANES), f32),
            pltpu.SemaphoreType.DMA((pieces,)),
        ],
        cost_estimate=pl.CostEstimate(flops=10**8, bytes_accessed=haps * variants * 4, transcendentals=0),
        compiler_params=pltpu.CompilerParams(vmem_limit_bytes=12 * MIB),
        name="count",
    )(panel)
    every_count = lax.all_to_all(counts, PANEL, 0, 0, tiled=True)

    turned, own = pl.pallas_call(
        turn_kernel,
        out_shape=(VMEM((variants, haps), bf16), VMEM((share, samples), f32)),
        in_specs=[whole(), pl.BlockSpec(memory_space=pl.ANY), pl.BlockSpec(memory_space=pl.ANY)],
        out_specs=(whole(), whole()),
        scratch_shapes=[
            VMEM((samples, LANES), jnp.int32),
            VMEM((samples, LANES), jnp.int32),
            VMEM((LANES, samples), f32),
            pltpu.SemaphoreType.DMA((2,)),
        ],
        cost_estimate=pl.CostEstimate(flops=10**9, bytes_accessed=haps * variants * 4, transcendentals=0),
        compiler_params=pltpu.CompilerParams(vmem_limit_bytes=4 * MIB),
        name="turn",
    )(as_bf16, called, present)

    mine, other = pl.pallas_call(
        functools.partial(impute_kernel, float(haps * devices)),
        out_shape=(VMEM((chips, height, LANES), f32), VMEM((chips, height, LANES), f32)),
        in_specs=[whole()] * 6,
        out_specs=(whole(), whole()),
        scratch_shapes=[
            VMEM((samples, variants), bf16),
            VMEM((samples, LANES), f32),
            VMEM((haps, samples), f32),
            VMEM((haps, samples), bf16),
        ],
        cost_estimate=pl.CostEstimate(
            flops=4 * samples * variants * haps, bytes_accessed=10**7, transcendentals=samples * haps
        ),
        compiler_params=pltpu.CompilerParams(vmem_limit_bytes=20 * MIB),
        name="impute",
    )(
        as_bf16,
        turned,
        every_count,
        in_vmem(called),
        in_vmem(present),
        sharpness.reshape(1, samples),
    )
    theirs = lax.ppermute(other, "panel_2", [(0, 1), (1, 0)])
    both = pl.pallas_call(
        pair_kernel,
        out_shape=VMEM((chips, height, LANES), f32),
        in_specs=[whole()] * 2,
        out_specs=whole(),
        cost_estimate=pl.CostEstimate(flops=10**7, bytes_accessed=10**6, transcendentals=0),
        compiler_params=pltpu.CompilerParams(vmem_limit_bytes=4 * MIB),
        name="pair",
    )(mine, theirs)
    parts = lax.all_to_all(both, CHIP_AXES, 0, 0, tiled=True)

    dose, stats = pl.pallas_call(
        dose_kernel,
        out_shape=(jax.ShapeDtypeStruct((share, samples), bf16), VMEM((strata, STATS, LANES), f32)),
        in_specs=[whole()] * 4,
        out_specs=(whole(), whole()),
        scratch_shapes=[VMEM((LANES, LANES), f32)],
        cost_estimate=pl.CostEstimate(flops=10**7, bytes_accessed=10**6, transcendentals=0),
        compiler_params=pltpu.CompilerParams(vmem_limit_bytes=6 * MIB),
        name="dose",
    )(parts, own, trait.reshape(1, samples), cohort.reshape(1, samples))
    every_stat = lax.all_to_all(stats, "samp", 0, 0, tiled=True)

    zscore = pl.pallas_call(
        functools.partial(score_kernel, float(samples * strata)),
        out_shape=jax.ShapeDtypeStruct((1, share), f32),
        in_specs=[whole()],
        out_specs=whole(),
        compiler_params=pltpu.CompilerParams(vmem_limit_bytes=4 * MIB),
        name="score",
    )(every_stat)
    return dose.T, zscore.reshape(share)


def solution(mesh):
    finer = Mesh(
        mesh.devices.reshape(4, 4, 2, mesh.shape["samp"]), ("panel_0", "panel_1", "panel_2", "samp")
    )
    placed = (P("samp", None), P("samp", None), P(PANEL, None), P("samp"), P("samp"), P("samp"))
    return jax.shard_map(
        on_device,
        mesh=finer,
        in_specs=placed,
        out_specs=(P("samp", PANEL), P(PANEL)),
        check_vma=False,
    )
```

```python
import functools

import jax
import jax.numpy as jnp
from jax import lax
from jax.experimental import pallas as pl
from jax.experimental.pallas import tpu as pltpu
from jax.sharding import Mesh
from jax.sharding import PartitionSpec as P

GROUPS = 8
CHIP_AXES = ("panel_0", "panel_1")
PANEL = ("panel_0", "panel_1", "panel_2")
LOG_TWO = 0.6931471805599453
LOG2_E = 1.4426950408889634
LANES = 128
STATS = 16
MIB = 1 << 20

VMEM = pltpu.VMEM


def in_vmem(x):
    return pltpu.with_memory_space_constraint(x, VMEM)


def in_hbm(x):
    return pltpu.with_memory_space_constraint(x, pltpu.HBM)


def whole():
    return pl.BlockSpec(memory_space=VMEM)


def count_kernel(
    panel,
    called,
    present,
    as_bf16,
    turned,
    counts,
    own,
    landed,
    tile,
    called_part,
    present_part,
    flipped,
    sems,
    own_sems,
):
    rows, variants = panel.shape
    pieces = sems.shape[0]
    step = rows // pieces

    def copy(i):
        span = pl.ds(pl.multiple_of(i * step, step), step)
        return pltpu.make_async_copy(panel.at[span], landed.at[span], sems.at[i])

    for i in range(pieces):
        copy(i).start()

    core = lax.axis_index("panel_2")
    here = (lax.axis_index("panel_0") * lax.axis_size("panel_1") + lax.axis_index("panel_1")) * 2
    here = here + core
    share = own.shape[0]
    per_tile = LANES // share
    lanes = pl.ds(pl.multiple_of((here // per_tile) * LANES, LANES), LANES)
    first = pltpu.make_async_copy(called.at[:, lanes], called_part, own_sems.at[0])
    second = pltpu.make_async_copy(present.at[:, lanes], present_part, own_sems.at[1])
    first.start()
    second.start()
    half = variants // 2

    def piece(i, acc):
        copy(i).wait()
        at = pl.ds(pl.multiple_of(i * step, step), step)
        for t in range(variants // LANES):
            cols = slice(t * LANES, (t + 1) * LANES)
            x = landed[at, cols]
            acc[t] = acc[t] + jnp.sum(x.reshape(step // 8, 8, LANES), axis=0)
            x = x.astype(jnp.float32).astype(jnp.bfloat16)
            as_bf16[at, cols] = x
            x = x.T
            for q in range(per_tile):
                chip = t * (per_tile // 2) + q // 2
                slot = jnp.bitwise_xor(core, q % 2)
                to = pl.ds(pl.multiple_of(slot * half + chip * share, share), share)
                turned[to, at] = x[q * share : (q + 1) * share, :]
        return acc

    zero = [jnp.zeros((8, LANES), jnp.int32) for _ in range(variants // LANES)]
    total = lax.fori_loop(0, pieces, piece, zero)
    for r in range(variants // LANES):
        tile[r : r + 1, :] = jnp.sum(total[r].astype(jnp.float32), axis=0, keepdims=True)
    one = tile[...]
    for j in range(counts.shape[0]):
        counts[j] = one
    first.wait()
    second.wait()
    code = jnp.where(present_part[...] == 1, called_part[...].astype(jnp.float32), -1.0)
    flipped[...] = code.T
    own[...] = flipped[pl.ds(pl.multiple_of((here % per_tile) * share, share), share), :]


def freq_row(counts, haplotypes, variants):
    total = jnp.sum(counts[...], axis=0)
    rows = [total[r : r + 1, :] for r in range(variants // LANES)]
    return jnp.concatenate(rows, axis=1) / haplotypes


def store_half(out, dose, steps, weight_total):
    tiles = dose.shape[1] // LANES
    blocks, height, _ = out.shape
    share = height // tiles - 2
    for t in range(tiles):
        lanes = slice(t * LANES, (t + 1) * LANES)
        for k in range(blocks):
            out[k, t * share : (t + 1) * share, :] = dose[k * share : (k + 1) * share, lanes]
        top = tiles * share + t
        out[0, top : top + 1, :] = steps[:, lanes]
        out[0, top + tiles : top + tiles + 1, :] = weight_total[:, lanes]


def impute_kernel(
    haplotypes,
    as_bf16,
    turned,
    counts,
    called,
    present,
    sharpness,
    other,
    weights,
    scales,
    centred,
    offsets,
    raw,
):
    samples, variants = called.shape
    haps = as_bf16.shape[0]
    tiles = samples // LANES
    freq = freq_row(counts, haplotypes, variants)
    twice = 2.0 * freq

    step = 64

    def centre(r, carry):
        span = pl.ds(pl.multiple_of(r * step, step), step)
        part = jnp.zeros((step, LANES), jnp.float32)
        for t in range(variants // LANES):
            cols = slice(t * LANES, (t + 1) * LANES)
            c = called[span, cols].astype(jnp.float32) - twice[:, cols]
            c = present[span, cols].astype(jnp.float32) * c
            c = c.astype(jnp.bfloat16)
            centred[span, cols] = c
            part += c.astype(jnp.float32) * freq[:, cols]
        offsets[span, :] = part
        return carry

    lax.fori_loop(0, samples // step, centre, 0)
    offset = jnp.concatenate(
        [
            jnp.sum(offsets[t * LANES : (t + 1) * LANES, :].T, axis=0, keepdims=True)
            for t in range(tiles)
        ],
        axis=1,
    )

    raw[...] = lax.dot_general(
        as_bf16[...], centred[...], (((1,), (1,)), ((), ())), preferred_element_type=jnp.float32
    )

    chunk = 128

    def highest(r, best):
        x = raw[pl.ds(pl.multiple_of(r * chunk, chunk), chunk), :]
        return jnp.maximum(best, jnp.max(x.reshape(chunk // 8, 8, samples), axis=0))

    best = lax.fori_loop(
        0, haps // chunk, highest, jnp.full((8, samples), -jnp.inf, jnp.float32)
    )
    best = jnp.max(best, axis=0, keepdims=True)
    heat = sharpness[...]
    peak = heat * (best - offset)
    steps = jnp.ceil(peak / LOG_TWO)
    slope = heat * LOG2_E
    shift = peak * LOG2_E - steps

    def weigh(r, acc):
        span = pl.ds(pl.multiple_of(r * chunk, chunk), chunk)
        w = jnp.exp2(slope * (raw[span, :] - best) + shift)
        weights[span, :] = w.astype(jnp.bfloat16)
        return acc + jnp.sum(w.reshape(chunk // 8, 8, samples), axis=0)

    acc = lax.fori_loop(0, haps // chunk, weigh, jnp.zeros((8, samples), jnp.float32))
    weight_total = jnp.sum(acc, axis=0, keepdims=True)
    scales[0:1, :] = steps
    scales[1:2, :] = weight_total
    dose = jnp.dot(
        turned[variants // 2 :, :], weights[...], preferred_element_type=jnp.float32
    )
    store_half(other, dose, steps, weight_total)


def mine_kernel(turned, weights, scales, mine):
    half = turned.shape[0] // 2
    dose = jnp.dot(turned[:half, :], weights[...], preferred_element_type=jnp.float32)
    store_half(mine, dose, scales[0:1, :], scales[1:2, :])


def pair_kernel(mine, theirs, both):
    blocks, height, _ = mine.shape
    tiles = 4
    share = height // tiles - 2
    top = tiles * share
    a, b = mine[0, top : top + tiles, :], theirs[0, top : top + tiles, :]
    steps = jnp.maximum(a, b)
    up, down = jnp.exp2(a - steps), jnp.exp2(b - steps)
    total = up * mine[0, top + tiles :, :] + down * theirs[0, top + tiles :, :]
    tail = jnp.concatenate([steps, total], axis=0)
    for k in range(blocks):
        for t in range(tiles):
            span = slice(t * share, (t + 1) * share)
            both[k, span, :] = (
                mine[k, span, :] * up[t : t + 1, :] + theirs[k, span, :] * down[t : t + 1, :]
            )
        both[k, top:, :] = tail


def dose_kernel(parts, own, trait, cohort, dose_out, stats, square):
    blocks, height, _ = parts.shape
    tiles = 4
    share = height // tiles - 2
    top = tiles * share
    sums = [jnp.zeros((share, LANES), jnp.float32) for _ in range(3 + GROUPS)]
    tail = [jnp.zeros((GROUPS, LANES), jnp.float32) for _ in range(3)]
    row = lax.broadcasted_iota(jnp.int32, (GROUPS, LANES), 0)
    steps = jnp.max(parts[:, top : top + tiles, :], axis=0)
    for t in range(tiles):
        lanes = slice(t * LANES, (t + 1) * LANES)
        peak = steps[t : t + 1, :]
        total = jnp.zeros((1, LANES), jnp.float32)
        dose = jnp.zeros((share, LANES), jnp.float32)
        for k in range(blocks):
            scale = jnp.exp2(parts[k, top + t : top + t + 1, :] - peak)
            total += scale * parts[k, top + tiles + t : top + tiles + t + 1, :]
            dose += scale * parts[k, t * share : (t + 1) * share, :]
        called = own[:, lanes]
        dose = jnp.where(called >= 0.0, called, 2.0 * dose / total)
        dose_out[:, lanes] = dose.astype(jnp.bfloat16)
        y, group = trait[:, lanes], cohort[:, lanes]
        sums[0] += y * dose
        sums[1] += dose
        sums[2] += dose * dose
        for g in range(GROUPS):
            sums[3 + g] += jnp.where(group == g, dose, 0.0)
        member = jnp.where(group == row, 1.0, 0.0)
        tail[0] += member * y
        tail[1] += member
        tail[2] += jnp.where(row == 0, y * y, 0.0)
    square[...] = jnp.zeros_like(square)
    lane = lax.broadcasted_iota(jnp.int32, (share, LANES), 1)
    packed = jnp.zeros((share, LANES), jnp.float32)
    for i, s in enumerate(sums):
        packed = jnp.where(lane == i, jnp.sum(s, axis=1, keepdims=True), packed)
    square[0:share, :] = packed
    lane = lax.broadcasted_iota(jnp.int32, (GROUPS, LANES), 1)
    packed = square[0:GROUPS, :]
    for i, s in enumerate(tail):
        packed = jnp.where(lane == 3 + GROUPS + i, jnp.sum(s, axis=1, keepdims=True), packed)
    square[0:GROUPS, :] = packed
    flat = square[...].T[0:STATS, :]
    for j in range(stats.shape[0]):
        stats[j] = flat


def score_kernel(all_samples, stats, zscore):
    s = jnp.sum(stats[...], axis=0)
    cross, dose_sum, dose_square = s[0:1, :], s[1:2, :], s[2:3, :]
    group_dose = s[3 : 3 + GROUPS, :]
    group_sum, group_count = s[3 + GROUPS : 4 + GROUPS, :], s[4 + GROUPS : 5 + GROUPS, :]
    lane = lax.broadcasted_iota(jnp.int32, (1, LANES), 1)
    group_mean = jnp.where(
        lane < GROUPS, group_sum / jnp.where(lane < GROUPS, group_count, 1.0), 0.0
    )
    row = lax.broadcasted_iota(jnp.int32, (GROUPS, LANES), 0)
    col = lax.broadcasted_iota(jnp.int32, (GROUPS, LANES), 1)
    means = jnp.sum(jnp.where(row == col, group_mean, 0.0), axis=1, keepdims=True)
    score_u = cross - jnp.sum(means * group_dose, axis=0, keepdims=True)
    explained = jnp.sum(
        jnp.where(lane < GROUPS, group_sum * group_mean, 0.0), axis=1, keepdims=True
    )
    square = s[5 + GROUPS : 6 + GROUPS, 0:1]
    sigma = (square - explained) / (all_samples - GROUPS)
    mean = dose_sum / all_samples
    spread = dose_square / all_samples - mean * mean
    z = score_u / jnp.sqrt(sigma * all_samples * (spread + 1e-05))
    zscore[...] = z[:, : zscore.shape[1]]


def on_device(called, present, panel, sharpness, trait, cohort):
    f32, bf16 = jnp.float32, jnp.bfloat16
    samples, variants = called.shape
    haps = panel.shape[0]
    devices = lax.axis_size(PANEL)
    chips = lax.axis_size(CHIP_AXES)
    strata = lax.axis_size("samp")
    tiles = samples // LANES
    share = variants // devices
    height = tiles * (share + 2)
    pieces = 16

    hbm = pl.BlockSpec(memory_space=pltpu.HBM)
    as_bf16, turned, counts, own = pl.pallas_call(
        count_kernel,
        out_shape=(
            VMEM((haps, variants), bf16),
            VMEM((variants, haps), bf16),
            VMEM((devices, 8, LANES), f32),
            VMEM((share, samples), f32),
        ),
        in_specs=[hbm] * 3,
        out_specs=(whole(),) * 4,
        scratch_shapes=[
            VMEM((haps, variants), jnp.int32),
            VMEM((8, LANES), f32),
            VMEM((samples, LANES), jnp.int32),
            VMEM((samples, LANES), jnp.int32),
            VMEM((LANES, samples), f32),
            pltpu.SemaphoreType.DMA((pieces,)),
            pltpu.SemaphoreType.DMA((2,)),
        ],
        cost_estimate=pl.CostEstimate(flops=10**9, bytes_accessed=haps * variants * 4, transcendentals=0),
        compiler_params=pltpu.CompilerParams(vmem_limit_bytes=14 * MIB),
        name="count",
    )(in_hbm(panel), in_hbm(called), in_hbm(present))
    every_count = lax.all_to_all(counts, PANEL, 0, 0, tiled=True)

    block = VMEM((chips, height, LANES), f32)
    other, weights, scales = pl.pallas_call(
        functools.partial(impute_kernel, float(haps * devices)),
        out_shape=(block, VMEM((haps, samples), bf16), VMEM((8, samples), f32)),
        in_specs=[whole()] * 6,
        out_specs=(whole(),) * 3,
        scratch_shapes=[
            VMEM((samples, variants), bf16),
            VMEM((samples, LANES), f32),
            VMEM((haps, samples), f32),
        ],
        cost_estimate=pl.CostEstimate(
            flops=3 * samples * variants * haps, bytes_accessed=10**7, transcendentals=samples * haps
        ),
        compiler_params=pltpu.CompilerParams(vmem_limit_bytes=16 * MIB),
        name="impute",
    )(
        as_bf16,
        turned,
        every_count,
        in_vmem(called),
        in_vmem(present),
        sharpness.reshape(1, samples),
    )
    theirs = lax.ppermute(other, "panel_2", [(0, 1), (1, 0)])
    mine = pl.pallas_call(
        mine_kernel,
        out_shape=block,
        in_specs=[whole()] * 3,
        out_specs=whole(),
        cost_estimate=pl.CostEstimate(
            flops=samples * variants * haps, bytes_accessed=10**6, transcendentals=0
        ),
        compiler_params=pltpu.CompilerParams(vmem_limit_bytes=4 * MIB),
        name="mine",
    )(turned, weights, scales)
    both = pl.pallas_call(
        pair_kernel,
        out_shape=VMEM((chips, height, LANES), f32),
        in_specs=[whole()] * 2,
        out_specs=whole(),
        cost_estimate=pl.CostEstimate(flops=10**7, bytes_accessed=10**6, transcendentals=0),
        compiler_params=pltpu.CompilerParams(vmem_limit_bytes=4 * MIB),
        name="pair",
    )(mine, theirs)
    parts = lax.all_to_all(both, CHIP_AXES, 0, 0, tiled=True)

    dose, stats = pl.pallas_call(
        dose_kernel,
        out_shape=(VMEM((share, samples), bf16), VMEM((strata, STATS, LANES), f32)),
        in_specs=[whole()] * 4,
        out_specs=(whole(), whole()),
        scratch_shapes=[VMEM((LANES, LANES), f32)],
        cost_estimate=pl.CostEstimate(flops=10**7, bytes_accessed=10**6, transcendentals=0),
        compiler_params=pltpu.CompilerParams(vmem_limit_bytes=6 * MIB),
        name="dose",
    )(parts, own, trait.reshape(1, samples), cohort.reshape(1, samples))
    every_stat = lax.all_to_all(stats, "samp", 0, 0, tiled=True)

    zscore = pl.pallas_call(
        functools.partial(score_kernel, float(samples * strata)),
        out_shape=jax.ShapeDtypeStruct((1, share), f32),
        in_specs=[whole()],
        out_specs=whole(),
        compiler_params=pltpu.CompilerParams(vmem_limit_bytes=4 * MIB),
        name="score",
    )(every_stat)
    return dose.T, zscore.reshape(share)


def solution(mesh):
    finer = Mesh(
        mesh.devices.reshape(4, 4, 2, mesh.shape["samp"]), ("panel_0", "panel_1", "panel_2", "samp")
    )
    placed = (P("samp", None), P("samp", None), P(PANEL, None), P("samp"), P("samp"), P("samp"))
    return jax.shard_map(
        on_device,
        mesh=finer,
        in_specs=placed,
        out_specs=(P("samp", PANEL), P(PANEL)),
        check_vma=False,
    )
```

```python
import functools

import jax
import jax.numpy as jnp
from jax import lax
from jax.experimental import pallas as pl
from jax.experimental.pallas import tpu as pltpu
from jax.sharding import Mesh
from jax.sharding import PartitionSpec as P

GROUPS = 8
CHIP_AXES = ("panel_0", "panel_1")
PANEL = ("panel_0", "panel_1", "panel_2")
LOG_TWO = 0.6931471805599453
LOG2_E = 1.4426950408889634
LANES = 128
STATS = 4
MIB = 1 << 20

VMEM = pltpu.VMEM


def in_vmem(x):
    return pltpu.with_memory_space_constraint(x, VMEM)


def in_hbm(x):
    return pltpu.with_memory_space_constraint(x, pltpu.HBM)


def whole():
    return pl.BlockSpec(memory_space=VMEM)


def count_kernel(panel, as_bf16, turned, counts, landed, tile, sems):
    rows, variants = panel.shape
    pieces = sems.shape[0]
    step = rows // pieces

    def copy(i):
        span = pl.ds(pl.multiple_of(i * step, step), step)
        return pltpu.make_async_copy(panel.at[span], landed.at[span], sems.at[i])

    for i in range(pieces):
        copy(i).start()

    core = lax.axis_index("panel_2")
    share = variants // counts.shape[0]
    per_tile = LANES // share
    half = variants // 2

    def piece(i, acc):
        copy(i).wait()
        at = pl.ds(pl.multiple_of(i * step, step), step)
        for t in range(variants // LANES):
            cols = slice(t * LANES, (t + 1) * LANES)
            x = landed[at, cols]
            acc[t] = acc[t] + jnp.sum(x.reshape(step // 8, 8, LANES), axis=0)
            x = x.astype(jnp.float32).astype(jnp.bfloat16)
            as_bf16[at, cols] = x
            x = x.T
            for q in range(per_tile):
                chip = t * (per_tile // 2) + q // 2
                slot = jnp.bitwise_xor(core, q % 2)
                to = pl.ds(pl.multiple_of(slot * half + chip * share, share), share)
                turned[to, at] = x[q * share : (q + 1) * share, :]
        return acc

    zero = [jnp.zeros((8, LANES), jnp.int32) for _ in range(variants // LANES)]
    total = lax.fori_loop(0, pieces, piece, zero)
    for r in range(variants // LANES):
        tile[r : r + 1, :] = jnp.sum(total[r].astype(jnp.float32), axis=0, keepdims=True)
    one = tile[...]
    for j in range(counts.shape[0]):
        counts[j] = one


def freq_row(counts, haplotypes, variants):
    total = jnp.sum(counts[...], axis=0)
    rows = [total[r : r + 1, :] for r in range(variants // LANES)]
    return jnp.concatenate(rows, axis=1) / haplotypes


def store_half(out, dose):
    tiles = dose.shape[1] // LANES
    share = out.shape[1] // tiles - 2
    for t in range(tiles):
        span = slice(t * share, (t + 1) * share)
        for k in range(out.shape[0]):
            out[k, span, :] = dose[k * share : (k + 1) * share, t * LANES : (t + 1) * LANES]


def store_tail(out, steps, weight_total):
    tiles = steps.shape[1] // LANES
    for t in range(tiles):
        lanes = slice(t * LANES, (t + 1) * LANES)
        top = out.shape[1] - 2 * tiles + t
        out[0, top : top + 1, :] = steps[:, lanes]
        out[0, top + tiles : top + tiles + 1, :] = weight_total[:, lanes]


def impute_kernel(
    haplotypes,
    as_bf16,
    turned,
    counts,
    called,
    present,
    sharpness,
    other,
    weights,
    scales,
    centred,
    offsets,
    raw,
):
    samples, variants = called.shape
    haps = as_bf16.shape[0]
    tiles = samples // LANES
    freq = freq_row(counts, haplotypes, variants)
    twice = 2.0 * freq

    step = 64

    def centre(r, carry):
        span = pl.ds(pl.multiple_of(r * step, step), step)
        part = jnp.zeros((step, LANES), jnp.float32)
        for t in range(variants // LANES):
            cols = slice(t * LANES, (t + 1) * LANES)
            c = called[span, cols].astype(jnp.float32) - twice[:, cols]
            c = present[span, cols].astype(jnp.float32) * c
            c = c.astype(jnp.bfloat16)
            centred[span, cols] = c
            part += c.astype(jnp.float32) * freq[:, cols]
        offsets[span, :] = part
        return carry

    lax.fori_loop(0, samples // step, centre, 0)
    offset = jnp.concatenate(
        [
            jnp.sum(offsets[t * LANES : (t + 1) * LANES, :].T, axis=0, keepdims=True)
            for t in range(tiles)
        ],
        axis=1,
    )

    product = lax.dot_general(
        as_bf16[...], centred[...], (((1,), (1,)), ((), ())), preferred_element_type=jnp.float32
    )
    raw[...] = product
    best = jnp.max(product.reshape(haps // 8, 8, samples), axis=0)
    best = jnp.max(best, axis=0, keepdims=True)
    heat = sharpness[...]
    peak = heat * (best - offset)
    steps = jnp.ceil(peak / LOG_TWO)
    slope = heat * LOG2_E
    shift = peak * LOG2_E - steps

    chunk = 128

    def weigh(r, acc):
        span = pl.ds(pl.multiple_of(r * chunk, chunk), chunk)
        w = jnp.exp2(slope * (raw[span, :] - best) + shift)
        weights[span, :] = w.astype(jnp.bfloat16)
        return acc + jnp.sum(w.reshape(chunk // 8, 8, samples), axis=0)

    acc = lax.fori_loop(0, haps // chunk, weigh, jnp.zeros((8, samples), jnp.float32))
    weight_total = jnp.sum(acc, axis=0, keepdims=True)
    scales[0:1, :] = steps
    scales[1:2, :] = weight_total
    dose = jnp.dot(turned[variants // 2 :, :], weights[...], preferred_element_type=jnp.float32)
    store_half(other, dose)
    store_tail(other, steps, weight_total)


def mine_kernel(
    turned, weights, scales, called, present, mine, own, called_part, present_part, flipped, sems
):
    here = (lax.axis_index("panel_0") * lax.axis_size("panel_1") + lax.axis_index("panel_1")) * 2
    here = here + lax.axis_index("panel_2")
    share = own.shape[0]
    per_tile = LANES // share
    lanes = pl.ds(pl.multiple_of((here // per_tile) * LANES, LANES), LANES)
    first = pltpu.make_async_copy(called.at[:, lanes], called_part, sems.at[0])
    second = pltpu.make_async_copy(present.at[:, lanes], present_part, sems.at[1])
    first.start()
    second.start()
    half = turned.shape[0] // 2
    dose = jnp.dot(turned[:half, :], weights[...], preferred_element_type=jnp.float32)
    store_half(mine, dose)
    store_tail(mine, scales[0:1, :], scales[1:2, :])
    first.wait()
    second.wait()
    code = jnp.where(present_part[...] == 1, called_part[...].astype(jnp.float32), -1.0)
    flipped[...] = code.T
    own[...] = flipped[pl.ds(pl.multiple_of((here % per_tile) * share, share), share), :]


def pair_kernel(mine, theirs, both):
    blocks, height, _ = mine.shape
    tiles = 4
    share = height // tiles - 2
    top = tiles * share
    a, b = mine[0, top : top + tiles, :], theirs[0, top : top + tiles, :]
    steps = jnp.maximum(a, b)
    up, down = jnp.exp2(a - steps), jnp.exp2(b - steps)
    total = up * mine[0, top + tiles :, :] + down * theirs[0, top + tiles :, :]
    tail = jnp.concatenate([steps, total], axis=0)
    for k in range(blocks):
        for t in range(tiles):
            span = slice(t * share, (t + 1) * share)
            both[k, span, :] = (
                mine[k, span, :] * up[t : t + 1, :] + theirs[k, span, :] * down[t : t + 1, :]
            )
        both[k, top:, :] = tail


def dose_kernel(parts, own, trait, cohort, rounded, stats, square):
    blocks, height, _ = parts.shape
    tiles = 4
    share = height // tiles - 2
    top = tiles * share
    sums = [jnp.zeros((share, LANES), jnp.float32) for _ in range(3 + GROUPS)]
    tail = [jnp.zeros((GROUPS, LANES), jnp.float32) for _ in range(3)]
    row = lax.broadcasted_iota(jnp.int32, (GROUPS, LANES), 0)
    steps = jnp.max(parts[:, top : top + tiles, :], axis=0)
    for t in range(tiles):
        lanes = slice(t * LANES, (t + 1) * LANES)
        peak = steps[t : t + 1, :]
        total = jnp.zeros((1, LANES), jnp.float32)
        dose = jnp.zeros((share, LANES), jnp.float32)
        for k in range(blocks):
            scale = jnp.exp2(parts[k, top + t : top + t + 1, :] - peak)
            total += scale * parts[k, top + tiles + t : top + tiles + t + 1, :]
            dose += scale * parts[k, t * share : (t + 1) * share, :]
        called = own[:, lanes]
        dose = jnp.where(called >= 0.0, called, 2.0 * dose / total)
        rounded[:, lanes] = dose.astype(jnp.bfloat16)
        y, group = trait[:, lanes], cohort[:, lanes]
        sums[0] += y * dose
        sums[1] += dose
        sums[2] += dose * dose
        for g in range(GROUPS):
            sums[3 + g] += jnp.where(group == g, dose, 0.0)
        member = jnp.where(group == row, 1.0, 0.0)
        tail[0] += member * y
        tail[1] += member
        tail[2] += jnp.where(row == 0, y * y, 0.0)
    sums = [jnp.sum(x, axis=1, keepdims=True) for x in sums]
    lane = lax.broadcasted_iota(jnp.int32, (share, LANES), 1)
    for q in range(LANES // share):
        packed = jnp.zeros((share, LANES), jnp.float32)
        for i in range(q, len(sums), LANES // share):
            packed = jnp.where(lane == i // (LANES // share), sums[i], packed)
        square[q * share : (q + 1) * share, :] = packed
    lane = lax.broadcasted_iota(jnp.int32, (GROUPS, LANES), 1)
    row, first = divmod(len(sums), LANES // share)
    for i, x in enumerate(tail):
        span = slice(first * share + i * GROUPS, first * share + (i + 1) * GROUPS)
        x = jnp.sum(x, axis=1, keepdims=True)
        square[span, :] = jnp.where(lane == row, x, square[span, :])
    flat = square[...].T[0:STATS, :]
    for j in range(stats.shape[0]):
        stats[j] = flat


def score_kernel(all_samples, stats, rounded, zscore, dose_out, line, sems):
    doses_leave = pltpu.make_async_copy(rounded, dose_out, sems.at[0])
    scores_leave = pltpu.make_async_copy(line, zscore, sems.at[1])
    doses_leave.start()
    share = zscore.shape[1]
    s = jnp.sum(stats[...], axis=0)
    parts = [s] + [pltpu.roll(s, LANES - q * share, axis=1) for q in range(1, LANES // share)]

    def stat(i):
        row, q = divmod(i, len(parts))
        return parts[q][row : row + 1, :]

    cross, dose_sum, dose_square = stat(0), stat(1), stat(2)
    group_dose = jnp.concatenate([stat(3 + g) for g in range(GROUPS)], axis=0)
    tail = stat(3 + GROUPS)
    lane = lax.broadcasted_iota(jnp.int32, (1, LANES), 1)
    row = lax.broadcasted_iota(jnp.int32, (GROUPS, LANES), 0)
    col = lax.broadcasted_iota(jnp.int32, (GROUPS, LANES), 1)
    group_sum = jnp.sum(jnp.where(col == row, tail, 0.0), axis=1, keepdims=True)
    group_count = jnp.sum(jnp.where(col == row + GROUPS, tail, 0.0), axis=1, keepdims=True)
    square = jnp.sum(jnp.where(lane == 2 * GROUPS, tail, 0.0), axis=1, keepdims=True)
    group_mean = group_sum / group_count
    score_u = cross - jnp.sum(group_mean * group_dose, axis=0, keepdims=True)
    explained = jnp.sum(group_sum * group_mean, axis=0, keepdims=True)
    sigma = (square - explained) / (all_samples - GROUPS)
    mean = dose_sum / all_samples
    spread = dose_square / all_samples - mean * mean
    z = score_u / jnp.sqrt(sigma * all_samples * (spread + 1e-05))
    line[...] = z[:, :share]
    scores_leave.start()
    doses_leave.wait()
    scores_leave.wait()


def on_device(called, present, panel, sharpness, trait, cohort):
    f32, bf16 = jnp.float32, jnp.bfloat16
    samples, variants = called.shape
    haps = panel.shape[0]
    devices = lax.axis_size(PANEL)
    chips = lax.axis_size(CHIP_AXES)
    strata = lax.axis_size("samp")
    tiles = samples // LANES
    share = variants // devices
    height = tiles * (share + 2)
    pieces = 16

    hbm = pl.BlockSpec(memory_space=pltpu.HBM)
    as_bf16, turned, counts = pl.pallas_call(
        count_kernel,
        out_shape=(
            VMEM((haps, variants), bf16),
            VMEM((variants, haps), bf16),
            VMEM((devices, 8, LANES), f32),
        ),
        in_specs=[hbm],
        out_specs=(whole(),) * 3,
        scratch_shapes=[
            VMEM((haps, variants), jnp.int32),
            VMEM((8, LANES), f32),
            pltpu.SemaphoreType.DMA((pieces,)),
        ],
        cost_estimate=pl.CostEstimate(flops=10**9, bytes_accessed=haps * variants * 4, transcendentals=0),
        compiler_params=pltpu.CompilerParams(vmem_limit_bytes=14 * MIB),
        name="count",
    )(in_hbm(panel))
    every_count = lax.all_to_all(counts, PANEL, 0, 0, tiled=True)

    block = VMEM((chips, height, LANES), f32)
    other, weights, scales = pl.pallas_call(
        functools.partial(impute_kernel, float(haps * devices)),
        out_shape=(block, VMEM((haps, samples), bf16), VMEM((8, samples), f32)),
        in_specs=[whole()] * 6,
        out_specs=(whole(),) * 3,
        scratch_shapes=[
            VMEM((samples, variants), bf16),
            VMEM((samples, LANES), f32),
            VMEM((haps, samples), f32),
        ],
        cost_estimate=pl.CostEstimate(
            flops=3 * samples * variants * haps, bytes_accessed=10**7, transcendentals=samples * haps
        ),
        compiler_params=pltpu.CompilerParams(vmem_limit_bytes=16 * MIB),
        name="impute",
    )(
        as_bf16,
        turned,
        every_count,
        in_vmem(called),
        in_vmem(present),
        sharpness.reshape(1, samples),
    )
    theirs = lax.ppermute(other, "panel_2", [(0, 1), (1, 0)])
    mine, own = pl.pallas_call(
        mine_kernel,
        out_shape=(block, VMEM((share, samples), f32)),
        in_specs=[whole()] * 3 + [hbm] * 2,
        out_specs=(whole(),) * 2,
        scratch_shapes=[
            VMEM((samples, LANES), jnp.int32),
            VMEM((samples, LANES), jnp.int32),
            VMEM((LANES, samples), f32),
            pltpu.SemaphoreType.DMA((2,)),
        ],
        cost_estimate=pl.CostEstimate(
            flops=samples * variants * haps, bytes_accessed=10**6, transcendentals=0
        ),
        compiler_params=pltpu.CompilerParams(vmem_limit_bytes=6 * MIB),
        name="mine",
    )(turned, weights, scales, in_hbm(called), in_hbm(present))
    both = pl.pallas_call(
        pair_kernel,
        out_shape=VMEM((chips, height, LANES), f32),
        in_specs=[whole()] * 2,
        out_specs=whole(),
        cost_estimate=pl.CostEstimate(flops=10**7, bytes_accessed=10**6, transcendentals=0),
        compiler_params=pltpu.CompilerParams(vmem_limit_bytes=4 * MIB),
        name="pair",
    )(mine, theirs)
    parts = lax.all_to_all(both, CHIP_AXES, 0, 0, tiled=True)

    rounded, stats = pl.pallas_call(
        dose_kernel,
        out_shape=(VMEM((share, samples), bf16), VMEM((strata, STATS, LANES), f32)),
        in_specs=[whole()] * 4,
        out_specs=(whole(), whole()),
        scratch_shapes=[VMEM((LANES, LANES), f32)],
        cost_estimate=pl.CostEstimate(flops=10**7, bytes_accessed=10**6, transcendentals=0),
        compiler_params=pltpu.CompilerParams(vmem_limit_bytes=6 * MIB),
        name="dose",
    )(parts, own, trait.reshape(1, samples), cohort.reshape(1, samples))
    every_stat = lax.all_to_all(stats, "samp", 0, 0, tiled=True)

    zscore, dose = pl.pallas_call(
        functools.partial(score_kernel, float(samples * strata)),
        out_shape=(pltpu.HBM((1, share), f32), pltpu.HBM((share, samples), bf16)),
        in_specs=[whole()] * 2,
        out_specs=(hbm, hbm),
        scratch_shapes=[VMEM((1, share), f32), pltpu.SemaphoreType.DMA((2,))],
        compiler_params=pltpu.CompilerParams(vmem_limit_bytes=4 * MIB),
        name="score",
    )(every_stat, rounded)
    return dose.T, zscore.reshape(share)


def solution(mesh):
    finer = Mesh(
        mesh.devices.reshape(4, 4, 2, mesh.shape["samp"]), ("panel_0", "panel_1", "panel_2", "samp")
    )
    placed = (P("samp", None), P("samp", None), P(PANEL, None), P("samp"), P("samp"), P("samp"))
    return jax.shard_map(
        on_device,
        mesh=finer,
        in_specs=placed,
        out_specs=(P("samp", PANEL), P(PANEL)),
        check_vma=False,
    )
```

```python
import functools

import jax
import jax.numpy as jnp
from jax import lax
from jax.experimental import pallas as pl
from jax.experimental.pallas import tpu as pltpu
from jax.sharding import Mesh
from jax.sharding import PartitionSpec as P

GROUPS = 8
CHIP_AXES = ("panel_0", "panel_1")
PANEL = ("panel_0", "panel_1", "panel_2")
LOG_TWO = 0.6931471805599453
LOG2_E = 1.4426950408889634
LANES = 128
STATS = 4
EXTRA = 16
MIB = 1 << 20

VMEM = pltpu.VMEM


def in_vmem(x):
    return pltpu.with_memory_space_constraint(x, VMEM)


def in_hbm(x):
    return pltpu.with_memory_space_constraint(x, pltpu.HBM)


def whole():
    return pl.BlockSpec(memory_space=VMEM)


def count_kernel(panel, as_bf16, turned, counts, landed, tile, sems):
    rows, variants = panel.shape
    pieces = sems.shape[0]
    step = rows // pieces

    def copy(i):
        span = pl.ds(pl.multiple_of(i * step, step), step)
        return pltpu.make_async_copy(panel.at[span], landed.at[span], sems.at[i])

    for i in range(pieces):
        copy(i).start()

    core = lax.axis_index("panel_2")
    share = variants // counts.shape[0]
    per_tile = LANES // share
    half = variants // 2

    def piece(i, acc):
        copy(i).wait()
        at = pl.ds(pl.multiple_of(i * step, step), step)
        for t in range(variants // LANES):
            cols = slice(t * LANES, (t + 1) * LANES)
            x = landed[at, cols]
            acc[t] = acc[t] + jnp.sum(x.reshape(step // 8, 8, LANES), axis=0)
            x = x.astype(jnp.float32).astype(jnp.bfloat16)
            as_bf16[at, cols] = x
            x = x.T
            for q in range(per_tile):
                chip = t * (per_tile // 2) + q // 2
                slot = jnp.bitwise_xor(core, q % 2)
                to = pl.ds(pl.multiple_of(slot * half + chip * share, share), share)
                turned[to, at] = x[q * share : (q + 1) * share, :]
        return acc

    zero = [jnp.zeros((8, LANES), jnp.int32) for _ in range(variants // LANES)]
    total = lax.fori_loop(0, pieces, piece, zero)
    for r in range(variants // LANES):
        tile[r : r + 1, :] = jnp.sum(total[r].astype(jnp.float32), axis=0, keepdims=True)
    one = tile[...]
    for j in range(counts.shape[0]):
        counts[j] = one


def freq_row(counts, haplotypes, variants):
    total = jnp.sum(counts[...], axis=0)
    rows = [total[r : r + 1, :] for r in range(variants // LANES)]
    return jnp.concatenate(rows, axis=1) / haplotypes


def store_half(out, dose):
    tiles = dose.shape[1] // LANES
    share = out.shape[1] // tiles - 2
    for t in range(tiles):
        span = slice(t * share, (t + 1) * share)
        for k in range(out.shape[0]):
            out[k, span, :] = dose[k * share : (k + 1) * share, t * LANES : (t + 1) * LANES]


def store_tail(out, steps, weight_total):
    tiles = steps.shape[1] // LANES
    for t in range(tiles):
        lanes = slice(t * LANES, (t + 1) * LANES)
        top = out.shape[1] - 2 * tiles + t
        out[0, top : top + 1, :] = steps[:, lanes]
        out[0, top + tiles : top + tiles + 1, :] = weight_total[:, lanes]


def impute_kernel(
    haplotypes,
    as_bf16,
    turned,
    counts,
    called,
    present,
    sharpness,
    other,
    weights,
    scales,
    centred,
    raw,
):
    samples, variants = called.shape
    haps = as_bf16.shape[0]
    freq = freq_row(counts, haplotypes, variants)
    twice = 2.0 * freq

    step = 64

    def centre(r, carry):
        span = pl.ds(pl.multiple_of(r * step, step), step)
        for t in range(variants // LANES):
            cols = slice(t * LANES, (t + 1) * LANES)
            c = called[span, cols].astype(jnp.float32) - twice[:, cols]
            c = jnp.where(present[span, cols] == 1, c, 0.0)
            centred[span, cols] = c.astype(jnp.bfloat16)
        return carry

    lax.fori_loop(0, samples // step, centre, 0)

    high = freq.astype(jnp.bfloat16).astype(jnp.float32)
    middle = (freq - high).astype(jnp.bfloat16).astype(jnp.float32)
    row = lax.broadcasted_iota(jnp.int32, (EXTRA, variants), 0)
    extra = jnp.where(row == 0, high, jnp.where(row == 1, middle, freq - high - middle))
    extra = jnp.where(row < 3, extra, 0.0).astype(jnp.bfloat16)
    product = lax.dot_general(
        jnp.concatenate([as_bf16[...], extra], axis=0),
        centred[...],
        (((1,), (1,)), ((), ())),
        preferred_element_type=jnp.float32,
    )
    offset = jnp.sum(product[haps:, :], axis=0, keepdims=True)
    product = product[:haps, :]
    raw[...] = product
    best = jnp.max(product.reshape(haps // 8, 8, samples), axis=0)
    best = jnp.max(best, axis=0, keepdims=True)
    heat = sharpness[...]
    peak = heat * (best - offset)
    steps = jnp.ceil(peak / LOG_TWO)
    slope = heat * LOG2_E
    shift = peak * LOG2_E - steps - slope * best

    chunk = 128

    def weigh(r, acc):
        span = pl.ds(pl.multiple_of(r * chunk, chunk), chunk)
        w = jnp.exp2(slope * raw[span, :] + shift)
        weights[span, :] = w.astype(jnp.bfloat16)
        return acc + jnp.sum(w.reshape(chunk // 8, 8, samples), axis=0)

    acc = lax.fori_loop(0, haps // chunk, weigh, jnp.zeros((8, samples), jnp.float32))
    weight_total = jnp.sum(acc, axis=0, keepdims=True)
    scales[0:1, :] = steps
    scales[1:2, :] = weight_total
    dose = jnp.dot(turned[variants // 2 :, :], weights[...], preferred_element_type=jnp.float32)
    store_half(other, dose)
    store_tail(other, steps, weight_total)


def mine_kernel(turned, weights, scales, called, present, mine, own, flipped):
    here = (lax.axis_index("panel_0") * lax.axis_size("panel_1") + lax.axis_index("panel_1")) * 2
    here = here + lax.axis_index("panel_2")
    share = own.shape[0]
    per_tile = LANES // share
    lanes = pl.ds(pl.multiple_of((here // per_tile) * LANES, LANES), LANES)
    code = jnp.where(present[:, lanes] == 1, called[:, lanes].astype(jnp.float32), -1.0)
    flipped[...] = code.T
    own[...] = flipped[pl.ds(pl.multiple_of((here % per_tile) * share, share), share), :]
    half = turned.shape[0] // 2
    dose = jnp.dot(turned[:half, :], weights[...], preferred_element_type=jnp.float32)
    store_half(mine, dose)
    store_tail(mine, scales[0:1, :], scales[1:2, :])


def pair_kernel(mine, theirs, both):
    blocks, height, _ = mine.shape
    tiles = 4
    share = height // tiles - 2
    top = tiles * share
    a, b = mine[0, top : top + tiles, :], theirs[0, top : top + tiles, :]
    steps = jnp.maximum(a, b)
    up, down = jnp.exp2(a - steps), jnp.exp2(b - steps)
    total = up * mine[0, top + tiles :, :] + down * theirs[0, top + tiles :, :]
    tail = jnp.concatenate([steps, total], axis=0)
    for k in range(blocks):
        for t in range(tiles):
            span = slice(t * share, (t + 1) * share)
            both[k, span, :] = (
                mine[k, span, :] * up[t : t + 1, :] + theirs[k, span, :] * down[t : t + 1, :]
            )
        both[k, top:, :] = tail


def dose_kernel(parts, own, trait, cohort, rounded, stats, square):
    blocks, height, _ = parts.shape
    tiles = 4
    share = height // tiles - 2
    top = tiles * share
    sums = [jnp.zeros((share, LANES), jnp.float32) for _ in range(3 + GROUPS)]
    tail = [jnp.zeros((GROUPS, LANES), jnp.float32) for _ in range(3)]
    row = lax.broadcasted_iota(jnp.int32, (GROUPS, LANES), 0)
    steps = jnp.max(parts[:, top : top + tiles, :], axis=0)
    for t in range(tiles):
        lanes = slice(t * LANES, (t + 1) * LANES)
        peak = steps[t : t + 1, :]
        total = jnp.zeros((1, LANES), jnp.float32)
        dose = jnp.zeros((share, LANES), jnp.float32)
        for k in range(blocks):
            scale = jnp.exp2(parts[k, top + t : top + t + 1, :] - peak)
            total += scale * parts[k, top + tiles + t : top + tiles + t + 1, :]
            dose += scale * parts[k, t * share : (t + 1) * share, :]
        called = own[:, lanes]
        dose = jnp.where(called >= 0.0, called, 2.0 * dose / total)
        rounded[:, lanes] = dose.astype(jnp.bfloat16)
        y, group = trait[:, lanes], cohort[:, lanes]
        sums[0] += y * dose
        sums[1] += dose
        sums[2] += dose * dose
        for g in range(GROUPS):
            sums[3 + g] += jnp.where(group == g, dose, 0.0)
        member = jnp.where(group == row, 1.0, 0.0)
        tail[0] += member * y
        tail[1] += member
        tail[2] += jnp.where(row == 0, y * y, 0.0)
    sums = [jnp.sum(x, axis=1, keepdims=True) for x in sums]
    lane = lax.broadcasted_iota(jnp.int32, (share, LANES), 1)
    for q in range(LANES // share):
        packed = jnp.zeros((share, LANES), jnp.float32)
        for i in range(q, len(sums), LANES // share):
            packed = jnp.where(lane == i // (LANES // share), sums[i], packed)
        square[q * share : (q + 1) * share, :] = packed
    lane = lax.broadcasted_iota(jnp.int32, (GROUPS, LANES), 1)
    row, first = divmod(len(sums), LANES // share)
    for i, x in enumerate(tail):
        span = slice(first * share + i * GROUPS, first * share + (i + 1) * GROUPS)
        x = jnp.sum(x, axis=1, keepdims=True)
        square[span, :] = jnp.where(lane == row, x, square[span, :])
    flat = square[...].T[0:STATS, :]
    for j in range(stats.shape[0]):
        stats[j] = flat


def score_kernel(all_samples, stats, rounded, zscore, dose_out, line, sems):
    doses_leave = pltpu.make_async_copy(rounded, dose_out, sems.at[0])
    scores_leave = pltpu.make_async_copy(line, zscore, sems.at[1])
    doses_leave.start()
    share = zscore.shape[1]
    s = jnp.sum(stats[...], axis=0)
    parts = [s] + [pltpu.roll(s, LANES - q * share, axis=1) for q in range(1, LANES // share)]

    def stat(i):
        row, q = divmod(i, len(parts))
        return parts[q][row : row + 1, :]

    cross, dose_sum, dose_square = stat(0), stat(1), stat(2)
    group_dose = jnp.concatenate([stat(3 + g) for g in range(GROUPS)], axis=0)
    tail = stat(3 + GROUPS)
    lane = lax.broadcasted_iota(jnp.int32, (1, LANES), 1)
    row = lax.broadcasted_iota(jnp.int32, (GROUPS, LANES), 0)
    col = lax.broadcasted_iota(jnp.int32, (GROUPS, LANES), 1)
    group_sum = jnp.sum(jnp.where(col == row, tail, 0.0), axis=1, keepdims=True)
    group_count = jnp.sum(jnp.where(col == row + GROUPS, tail, 0.0), axis=1, keepdims=True)
    square = jnp.sum(jnp.where(lane == 2 * GROUPS, tail, 0.0), axis=1, keepdims=True)
    group_mean = group_sum / group_count
    score_u = cross - jnp.sum(group_mean * group_dose, axis=0, keepdims=True)
    explained = jnp.sum(group_sum * group_mean, axis=0, keepdims=True)
    sigma = (square - explained) / (all_samples - GROUPS)
    mean = dose_sum / all_samples
    spread = dose_square / all_samples - mean * mean
    z = score_u / jnp.sqrt(sigma * all_samples * (spread + 1e-05))
    line[...] = z[:, :share]
    scores_leave.start()
    doses_leave.wait()
    scores_leave.wait()


def on_device(called, present, panel, sharpness, trait, cohort):
    f32, bf16 = jnp.float32, jnp.bfloat16
    samples, variants = called.shape
    haps = panel.shape[0]
    devices = lax.axis_size(PANEL)
    chips = lax.axis_size(CHIP_AXES)
    strata = lax.axis_size("samp")
    tiles = samples // LANES
    share = variants // devices
    height = tiles * (share + 2)
    pieces = 16

    hbm = pl.BlockSpec(memory_space=pltpu.HBM)
    as_bf16, turned, counts = pl.pallas_call(
        count_kernel,
        out_shape=(
            VMEM((haps, variants), bf16),
            VMEM((variants, haps), bf16),
            VMEM((devices, 8, LANES), f32),
        ),
        in_specs=[hbm],
        out_specs=(whole(),) * 3,
        scratch_shapes=[
            VMEM((haps, variants), jnp.int32),
            VMEM((8, LANES), f32),
            pltpu.SemaphoreType.DMA((pieces,)),
        ],
        cost_estimate=pl.CostEstimate(flops=10**9, bytes_accessed=haps * variants * 4, transcendentals=0),
        compiler_params=pltpu.CompilerParams(vmem_limit_bytes=14 * MIB),
        name="count",
    )(in_hbm(panel))
    every_count = lax.all_to_all(counts, PANEL, 0, 0, tiled=True)

    block = VMEM((chips, height, LANES), f32)
    called_near, present_near = in_vmem(called), in_vmem(present)
    other, weights, scales = pl.pallas_call(
        functools.partial(impute_kernel, float(haps * devices)),
        out_shape=(block, VMEM((haps, samples), bf16), VMEM((8, samples), f32)),
        in_specs=[whole()] * 6,
        out_specs=(whole(),) * 3,
        scratch_shapes=[
            VMEM((samples, variants), bf16),
            VMEM((haps, samples), f32),
        ],
        cost_estimate=pl.CostEstimate(
            flops=3 * samples * variants * haps, bytes_accessed=10**7, transcendentals=samples * haps
        ),
        compiler_params=pltpu.CompilerParams(vmem_limit_bytes=16 * MIB),
        name="impute",
    )(
        as_bf16,
        turned,
        every_count,
        called_near,
        present_near,
        sharpness.reshape(1, samples),
    )
    theirs = lax.ppermute(other, "panel_2", [(0, 1), (1, 0)])
    mine, own = pl.pallas_call(
        mine_kernel,
        out_shape=(block, VMEM((share, samples), f32)),
        in_specs=[whole()] * 5,
        out_specs=(whole(),) * 2,
        scratch_shapes=[VMEM((LANES, samples), f32)],
        cost_estimate=pl.CostEstimate(
            flops=samples * variants * haps, bytes_accessed=10**6, transcendentals=0
        ),
        compiler_params=pltpu.CompilerParams(vmem_limit_bytes=6 * MIB),
        name="mine",
    )(turned, weights, scales, called_near, present_near)
    both = pl.pallas_call(
        pair_kernel,
        out_shape=VMEM((chips, height, LANES), f32),
        in_specs=[whole()] * 2,
        out_specs=whole(),
        cost_estimate=pl.CostEstimate(flops=10**7, bytes_accessed=10**6, transcendentals=0),
        compiler_params=pltpu.CompilerParams(vmem_limit_bytes=4 * MIB),
        name="pair",
    )(mine, theirs)
    parts = lax.all_to_all(both, CHIP_AXES, 0, 0, tiled=True)

    rounded, stats = pl.pallas_call(
        dose_kernel,
        out_shape=(VMEM((share, samples), bf16), VMEM((strata, STATS, LANES), f32)),
        in_specs=[whole()] * 4,
        out_specs=(whole(), whole()),
        scratch_shapes=[VMEM((LANES, LANES), f32)],
        cost_estimate=pl.CostEstimate(flops=10**7, bytes_accessed=10**6, transcendentals=0),
        compiler_params=pltpu.CompilerParams(vmem_limit_bytes=6 * MIB),
        name="dose",
    )(parts, own, trait.reshape(1, samples), cohort.reshape(1, samples))
    every_stat = lax.all_to_all(stats, "samp", 0, 0, tiled=True)

    zscore, dose = pl.pallas_call(
        functools.partial(score_kernel, float(samples * strata)),
        out_shape=(pltpu.HBM((1, share), f32), pltpu.HBM((share, samples), bf16)),
        in_specs=[whole()] * 2,
        out_specs=(hbm, hbm),
        scratch_shapes=[VMEM((1, share), f32), pltpu.SemaphoreType.DMA((2,))],
        compiler_params=pltpu.CompilerParams(vmem_limit_bytes=4 * MIB),
        name="score",
    )(every_stat, rounded)
    return dose.T, zscore.reshape(share)


def solution(mesh):
    finer = Mesh(
        mesh.devices.reshape(4, 4, 2, mesh.shape["samp"]), ("panel_0", "panel_1", "panel_2", "samp")
    )
    placed = (P("samp", None), P("samp", None), P(PANEL, None), P("samp"), P("samp"), P("samp"))
    return jax.shard_map(
        on_device,
        mesh=finer,
        in_specs=placed,
        out_specs=(P("samp", PANEL), P(PANEL)),
        check_vma=False,
    )
```

```python
import functools

import jax
import jax.numpy as jnp
from jax import lax
from jax.experimental import pallas as pl
from jax.experimental.pallas import tpu as pltpu
from jax.sharding import Mesh
from jax.sharding import PartitionSpec as P

GROUPS = 8
CHIP_AXES = ("panel_0", "panel_1")
PANEL = ("panel_0", "panel_1", "panel_2")
LOG_TWO = 0.6931471805599453
LOG2_E = 1.4426950408889634
LANES = 128
STATS = 4
EXTRA = 16
MIB = 1 << 20

VMEM = pltpu.VMEM


def in_vmem(x):
    return pltpu.with_memory_space_constraint(x, VMEM)


def in_hbm(x):
    return pltpu.with_memory_space_constraint(x, pltpu.HBM)


def whole():
    return pl.BlockSpec(memory_space=VMEM)


def count_kernel(panel, as_bf16, turned, counts, landed, tile, sems):
    rows, variants = panel.shape
    pieces = sems.shape[0]
    step = rows // pieces

    def copy(i):
        span = pl.ds(pl.multiple_of(i * step, step), step)
        return pltpu.make_async_copy(panel.at[span], landed.at[span], sems.at[i])

    for i in range(pieces):
        copy(i).start()

    core = lax.axis_index("panel_2")
    share = variants // counts.shape[0]
    per_tile = LANES // share
    half = variants // 2

    def piece(i, acc):
        copy(i).wait()
        at = pl.ds(pl.multiple_of(i * step, step), step)
        for t in range(variants // LANES):
            cols = slice(t * LANES, (t + 1) * LANES)
            x = landed[at, cols]
            acc[t] = acc[t] + jnp.sum(x.reshape(step // 8, 8, LANES), axis=0)
            x = x.astype(jnp.float32).astype(jnp.bfloat16)
            as_bf16[at, cols] = x
            x = x.T
            for q in range(per_tile):
                chip = t * (per_tile // 2) + q // 2
                slot = jnp.bitwise_xor(core, q % 2)
                to = pl.ds(pl.multiple_of(slot * half + chip * share, share), share)
                turned[to, at] = x[q * share : (q + 1) * share, :]
        return acc

    zero = [jnp.zeros((8, LANES), jnp.int32) for _ in range(variants // LANES)]
    total = lax.fori_loop(0, pieces, piece, zero)
    for r in range(variants // LANES):
        tile[r : r + 1, :] = jnp.sum(total[r].astype(jnp.float32), axis=0, keepdims=True)
    one = tile[...]
    for j in range(counts.shape[0]):
        counts[j] = one


def freq_row(counts, haplotypes, variants):
    total = jnp.sum(counts[...], axis=0)
    rows = [total[r : r + 1, :] for r in range(variants // LANES)]
    return jnp.concatenate(rows, axis=1) / haplotypes


def store_half(out, dose):
    tiles = dose.shape[1] // LANES
    share = out.shape[1] // tiles - 2
    for t in range(tiles):
        span = slice(t * share, (t + 1) * share)
        for k in range(out.shape[0]):
            out[k, span, :] = dose[k * share : (k + 1) * share, t * LANES : (t + 1) * LANES]


def store_tail(out, steps, weight_total):
    tiles = steps.shape[1] // LANES
    for t in range(tiles):
        lanes = slice(t * LANES, (t + 1) * LANES)
        top = out.shape[1] - 2 * tiles + t
        out[0, top : top + 1, :] = steps[:, lanes]
        out[0, top + tiles : top + tiles + 1, :] = weight_total[:, lanes]


def impute_kernel(
    haplotypes,
    chips,
    as_bf16,
    turned,
    counts,
    called,
    present,
    sharpness,
    other,
    weights,
    scales,
    centred,
    raw,
):
    samples, variants = called.shape
    haps = as_bf16.shape[0]
    freq = freq_row(counts, haplotypes, variants)
    twice = 2.0 * freq

    step = 128

    def centre(r, carry):
        span = pl.ds(pl.multiple_of(r * step, step), step)
        for t in range(variants // LANES):
            cols = slice(t * LANES, (t + 1) * LANES)
            c = called[span, cols].astype(jnp.float32) - twice[:, cols]
            c = jnp.where(present[span, cols] == 1, c, 0.0)
            centred[span, cols] = c.astype(jnp.bfloat16)
        return carry

    lax.fori_loop(0, samples // step, centre, 0)

    high = freq.astype(jnp.bfloat16).astype(jnp.float32)
    middle = (freq - high).astype(jnp.bfloat16).astype(jnp.float32)
    row = lax.broadcasted_iota(jnp.int32, (EXTRA, variants), 0)
    extra = jnp.where(row == 0, high, jnp.where(row == 1, middle, freq - high - middle))
    extra = jnp.where(row < 3, extra, 0.0).astype(jnp.bfloat16)
    product = lax.dot_general(
        jnp.concatenate([as_bf16[...], extra], axis=0),
        centred[...],
        (((1,), (1,)), ((), ())),
        preferred_element_type=jnp.float32,
    )
    offset = jnp.sum(product[haps:, :], axis=0, keepdims=True)
    product = product[:haps, :]
    raw[...] = product
    best = jnp.max(product.reshape(haps // 8, 8, samples), axis=0)
    best = jnp.max(best, axis=0, keepdims=True)
    heat = sharpness[...]
    peak = heat * (best - offset)
    steps = jnp.ceil(peak / LOG_TWO)
    slope = heat * LOG2_E
    shift = peak * LOG2_E - steps - slope * best

    chunk = 256

    def weigh(r, acc):
        span = pl.ds(pl.multiple_of(r * chunk, chunk), chunk)
        w = jnp.exp2(slope * raw[span, :] + shift)
        weights[span, :] = w.astype(jnp.bfloat16)
        return acc + jnp.sum(w.reshape(chunk // 8, 8, samples), axis=0)

    acc = lax.fori_loop(0, haps // chunk, weigh, jnp.zeros((8, samples), jnp.float32))
    weight_total = jnp.sum(acc, axis=0, keepdims=True)
    scales[0:1, :] = steps
    scales[1:2, :] = weight_total
    dose = jnp.dot(turned[variants // 2 :, :], weights[...], preferred_element_type=jnp.float32)
    share = variants // 2 // chips
    tiles = samples // LANES
    for t in range(tiles):
        lanes = slice(t * LANES, (t + 1) * LANES)
        for k in range(chips):
            at = (k * tiles + t) * share
            other[at : at + share, :] = dose[k * share : (k + 1) * share, lanes]
        top = tiles * chips * share + t
        other[top : top + 1, :] = steps[:, lanes]
        other[top + tiles : top + tiles + 1, :] = weight_total[:, lanes]


def mine_kernel(turned, weights, scales, called, present, mine, own, flipped):
    here = (lax.axis_index("panel_0") * lax.axis_size("panel_1") + lax.axis_index("panel_1")) * 2
    here = here + lax.axis_index("panel_2")
    share = own.shape[0]
    per_tile = LANES // share
    lanes = pl.ds(pl.multiple_of((here // per_tile) * LANES, LANES), LANES)
    code = jnp.where(present[:, lanes] == 1, called[:, lanes].astype(jnp.float32), -1.0)
    flipped[...] = code.T
    own[...] = flipped[pl.ds(pl.multiple_of((here % per_tile) * share, share), share), :]
    half = turned.shape[0] // 2
    dose = jnp.dot(turned[:half, :], weights[...], preferred_element_type=jnp.float32)
    store_half(mine, dose)
    store_tail(mine, scales[0:1, :], scales[1:2, :])


def pair_kernel(mine, theirs, both):
    blocks, height, _ = mine.shape
    tiles = 4
    share = height // tiles - 2
    top = tiles * share
    end = blocks * top
    a, b = mine[0, top : top + tiles, :], theirs[end : end + tiles, :]
    steps = jnp.maximum(a, b)
    up, down = jnp.exp2(a - steps), jnp.exp2(b - steps)
    total = up * mine[0, top + tiles :, :] + down * theirs[end + tiles :, :]
    tail = jnp.concatenate([steps, total], axis=0)
    for k in range(blocks):
        for t in range(tiles):
            span = slice(t * share, (t + 1) * share)
            x = theirs[k * top + t * share : k * top + (t + 1) * share, :]
            both[k, span, :] = mine[k, span, :] * up[t : t + 1, :] + x * down[t : t + 1, :]
        both[k, top:, :] = tail


def dose_kernel(parts, own, trait, cohort, rounded, stats, square):
    blocks, height, _ = parts.shape
    tiles = 4
    share = height // tiles - 2
    top = tiles * share
    sums = [jnp.zeros((share, LANES), jnp.float32) for _ in range(3 + GROUPS)]
    tail = [jnp.zeros((GROUPS, LANES), jnp.float32) for _ in range(3)]
    row = lax.broadcasted_iota(jnp.int32, (GROUPS, LANES), 0)
    steps = jnp.max(parts[:, top : top + tiles, :], axis=0)
    for t in range(tiles):
        lanes = slice(t * LANES, (t + 1) * LANES)
        peak = steps[t : t + 1, :]
        total = jnp.zeros((1, LANES), jnp.float32)
        dose = jnp.zeros((share, LANES), jnp.float32)
        for k in range(blocks):
            scale = jnp.exp2(parts[k, top + t : top + t + 1, :] - peak)
            total += scale * parts[k, top + tiles + t : top + tiles + t + 1, :]
            dose += scale * parts[k, t * share : (t + 1) * share, :]
        called = own[:, lanes]
        dose = jnp.where(called >= 0.0, called, 2.0 * dose / total)
        rounded[:, lanes] = dose.astype(jnp.bfloat16)
        y, group = trait[:, lanes], cohort[:, lanes]
        sums[0] += y * dose
        sums[1] += dose
        sums[2] += dose * dose
        for g in range(GROUPS):
            sums[3 + g] += jnp.where(group == g, dose, 0.0)
        member = jnp.where(group == row, 1.0, 0.0)
        tail[0] += member * y
        tail[1] += member
        tail[2] += jnp.where(row == 0, y * y, 0.0)
    sums = [jnp.sum(x, axis=1, keepdims=True) for x in sums]
    lane = lax.broadcasted_iota(jnp.int32, (share, LANES), 1)
    for q in range(LANES // share):
        packed = jnp.zeros((share, LANES), jnp.float32)
        for i in range(q, len(sums), LANES // share):
            packed = jnp.where(lane == i // (LANES // share), sums[i], packed)
        square[q * share : (q + 1) * share, :] = packed
    lane = lax.broadcasted_iota(jnp.int32, (GROUPS, LANES), 1)
    row, first = divmod(len(sums), LANES // share)
    for i, x in enumerate(tail):
        span = slice(first * share + i * GROUPS, first * share + (i + 1) * GROUPS)
        x = jnp.sum(x, axis=1, keepdims=True)
        square[span, :] = jnp.where(lane == row, x, square[span, :])
    flat = square[...].T[0:STATS, :]
    for j in range(stats.shape[0]):
        stats[j] = flat


def score_kernel(all_samples, stats, rounded, zscore, dose_out, line, sems):
    doses_leave = pltpu.make_async_copy(rounded, dose_out, sems.at[0])
    scores_leave = pltpu.make_async_copy(line, zscore, sems.at[1])
    doses_leave.start()
    share = zscore.shape[1]
    s = jnp.sum(stats[...], axis=0)
    parts = [s] + [pltpu.roll(s, LANES - q * share, axis=1) for q in range(1, LANES // share)]

    def stat(i):
        row, q = divmod(i, len(parts))
        return parts[q][row : row + 1, :]

    cross, dose_sum, dose_square = stat(0), stat(1), stat(2)
    group_dose = jnp.concatenate([stat(3 + g) for g in range(GROUPS)], axis=0)
    tail = stat(3 + GROUPS)
    lane = lax.broadcasted_iota(jnp.int32, (1, LANES), 1)
    row = lax.broadcasted_iota(jnp.int32, (GROUPS, LANES), 0)
    col = lax.broadcasted_iota(jnp.int32, (GROUPS, LANES), 1)
    group_sum = jnp.sum(jnp.where(col == row, tail, 0.0), axis=1, keepdims=True)
    group_count = jnp.sum(jnp.where(col == row + GROUPS, tail, 0.0), axis=1, keepdims=True)
    square = jnp.sum(jnp.where(lane == 2 * GROUPS, tail, 0.0), axis=1, keepdims=True)
    group_mean = group_sum / group_count
    score_u = cross - jnp.sum(group_mean * group_dose, axis=0, keepdims=True)
    explained = jnp.sum(group_sum * group_mean, axis=0, keepdims=True)
    sigma = (square - explained) / (all_samples - GROUPS)
    mean = dose_sum / all_samples
    spread = dose_square / all_samples - mean * mean
    z = score_u / jnp.sqrt(sigma * all_samples * (spread + 1e-05))
    line[...] = z[:, :share]
    scores_leave.start()
    doses_leave.wait()
    scores_leave.wait()


def on_device(called, present, panel, sharpness, trait, cohort):
    f32, bf16 = jnp.float32, jnp.bfloat16
    samples, variants = called.shape
    haps = panel.shape[0]
    devices = lax.axis_size(PANEL)
    chips = lax.axis_size(CHIP_AXES)
    strata = lax.axis_size("samp")
    tiles = samples // LANES
    share = variants // devices
    height = tiles * (share + 2)
    pieces = 16

    hbm = pl.BlockSpec(memory_space=pltpu.HBM)
    as_bf16, turned, counts = pl.pallas_call(
        count_kernel,
        out_shape=(
            VMEM((haps, variants), bf16),
            VMEM((variants, haps), bf16),
            VMEM((devices, 8, LANES), f32),
        ),
        in_specs=[hbm],
        out_specs=(whole(),) * 3,
        scratch_shapes=[
            VMEM((haps, variants), jnp.int32),
            VMEM((8, LANES), f32),
            pltpu.SemaphoreType.DMA((pieces,)),
        ],
        cost_estimate=pl.CostEstimate(flops=10**9, bytes_accessed=haps * variants * 4, transcendentals=0),
        compiler_params=pltpu.CompilerParams(vmem_limit_bytes=14 * MIB),
        name="count",
    )(in_hbm(panel))
    every_count = lax.all_to_all(counts, PANEL, 0, 0, tiled=True)

    block = VMEM((chips, height, LANES), f32)
    called_near, present_near = in_vmem(called), in_vmem(present)
    other, weights, scales = pl.pallas_call(
        functools.partial(impute_kernel, float(haps * devices), chips),
        out_shape=(
            VMEM((chips * tiles * share + 2 * tiles, LANES), f32),
            VMEM((haps, samples), bf16),
            VMEM((8, samples), f32),
        ),
        in_specs=[whole()] * 6,
        out_specs=(whole(),) * 3,
        scratch_shapes=[
            VMEM((samples, variants), bf16),
            VMEM((haps, samples), f32),
        ],
        cost_estimate=pl.CostEstimate(
            flops=3 * samples * variants * haps, bytes_accessed=10**7, transcendentals=samples * haps
        ),
        compiler_params=pltpu.CompilerParams(vmem_limit_bytes=16 * MIB),
        name="impute",
    )(
        as_bf16,
        turned,
        every_count,
        called_near,
        present_near,
        sharpness.reshape(1, samples),
    )
    theirs = lax.ppermute(other, "panel_2", [(0, 1), (1, 0)])
    mine, own = pl.pallas_call(
        mine_kernel,
        out_shape=(block, VMEM((share, samples), f32)),
        in_specs=[whole()] * 5,
        out_specs=(whole(),) * 2,
        scratch_shapes=[VMEM((LANES, samples), f32)],
        cost_estimate=pl.CostEstimate(
            flops=samples * variants * haps, bytes_accessed=10**6, transcendentals=0
        ),
        compiler_params=pltpu.CompilerParams(vmem_limit_bytes=6 * MIB),
        name="mine",
    )(turned, weights, scales, called_near, present_near)
    both = pl.pallas_call(
        pair_kernel,
        out_shape=VMEM((chips, height, LANES), f32),
        in_specs=[whole()] * 2,
        out_specs=whole(),
        cost_estimate=pl.CostEstimate(flops=10**7, bytes_accessed=10**6, transcendentals=0),
        compiler_params=pltpu.CompilerParams(vmem_limit_bytes=4 * MIB),
        name="pair",
    )(mine, theirs)
    parts = lax.all_to_all(both, CHIP_AXES, 0, 0, tiled=True)

    rounded, stats = pl.pallas_call(
        dose_kernel,
        out_shape=(VMEM((share, samples), bf16), VMEM((strata, STATS, LANES), f32)),
        in_specs=[whole()] * 4,
        out_specs=(whole(), whole()),
        scratch_shapes=[VMEM((LANES, LANES), f32)],
        cost_estimate=pl.CostEstimate(flops=10**7, bytes_accessed=10**6, transcendentals=0),
        compiler_params=pltpu.CompilerParams(vmem_limit_bytes=6 * MIB),
        name="dose",
    )(parts, own, trait.reshape(1, samples), cohort.reshape(1, samples))
    every_stat = lax.all_to_all(stats, "samp", 0, 0, tiled=True)

    zscore, dose = pl.pallas_call(
        functools.partial(score_kernel, float(samples * strata)),
        out_shape=(pltpu.HBM((1, share), f32), pltpu.HBM((share, samples), bf16)),
        in_specs=[whole()] * 2,
        out_specs=(hbm, hbm),
        scratch_shapes=[VMEM((1, share), f32), pltpu.SemaphoreType.DMA((2,))],
        compiler_params=pltpu.CompilerParams(vmem_limit_bytes=4 * MIB),
        name="score",
    )(every_stat, rounded)
    return dose.T, zscore.reshape(share)


def solution(mesh):
    finer = Mesh(
        mesh.devices.reshape(4, 4, 2, mesh.shape["samp"]), ("panel_0", "panel_1", "panel_2", "samp")
    )
    placed = (P("samp", None), P("samp", None), P(PANEL, None), P("samp"), P("samp"), P("samp"))
    return jax.shard_map(
        on_device,
        mesh=finer,
        in_specs=placed,
        out_specs=(P("samp", PANEL), P(PANEL)),
        check_vma=False,
    )
```
